16 devices in a mesh: rep: 1, dp: 16 (over x, y, z, core).
Axes of the slice: x: 2, y: 2, z: 2, core: 2. Of those that a mesh axis runs over, the one named last changes fastest.
Arguments:
- x: bfloat16 [16, 2048, 1536], P(('rep', 'dp'))
- dy: bfloat16 [16, 2048, 1536], P(('rep', 'dp'))
- w_gate: bfloat16 [2, 1536, 4224], replicated
- w_up: bfloat16 [2, 1536, 4224], replicated
- w_down: bfloat16 [2, 4224, 1536], replicated
- m_w_gate: float32 [2, 1536, 4224], P(None, 'dp')
- m_w_up: float32 [2, 1536, 4224], P(None, 'dp')
- m_w_down: float32 [2, 4224, 1536], P(None, 'dp')
- v_w_gate: float32 [2, 1536, 4224], P(None, 'dp')
- v_w_up: float32 [2, 1536, 4224], P(None, 'dp')
- v_w_down: float32 [2, 4224, 1536], P(None, 'dp')
Outputs:
- output 1: bfloat16 [2, 1536, 4224], P('rep')
- output 2: bfloat16 [2, 1536, 4224], P('rep')
- output 3: bfloat16 [2, 4224, 1536], P('rep')
- output 4: float32 [2, 1536, 4224], P('rep', 'dp')
- output 5: float32 [2, 1536, 4224], P('rep', 'dp')
- output 6: float32 [2, 4224, 1536], P('rep', 'dp')
- output 7: float32 [2, 1536, 4224], P('rep', 'dp')
- output 8: float32 [2, 1536, 4224], P('rep', 'dp')
- output 9: float32 [2, 4224, 1536], P('rep', 'dp')
All inputs are finite; a program needn't handle non-finite values.
Results may differ from the reference program's by a relative error of at most 0.022.
Values are sent between devices in bfloat16 or wider.
A program may use at most 2 GiB of HBM per device.

```python
import jax
import jax.numpy as jnp
from jax import lax

SEQUENCES = 16
TOKENS = 2048
D = 1536
FF = 4224
LAYERS = 2
NAMES = ("w_gate", "w_up", "w_down")
SHAPES = {"w_gate": (LAYERS, D, FF), "w_up": (LAYERS, D, FF), "w_down": (LAYERS, FF, D)}


def bump(key, n, height):
    away = (jnp.arange(n, dtype=jnp.int32) - jax.random.randint(key, (), 0, n, jnp.int32)) % n
    return jnp.where(away < n // 8, height, 1.0)


def together(key, own, strength):
    shared = jax.random.normal(key, own.shape[1:], jnp.float32)
    return (own + strength * shared) * lax.rsqrt(1 + strength * strength)


def setup_inputs(seed: int = 0, part: int = 0) -> dict:
    kx, kdy, ka, kb, kz, kf, kh, kl, *keys = jax.random.split(jax.random.key(seed), 8 + 3 * len(NAMES))
    kx, kdy, ka, kb = (jax.random.fold_in(k, part) for k in (kx, kdy, ka, kb))
    kw, km, kv = (keys[i::3] for i in range(3))
    shape = (SEQUENCES, TOKENS, D)
    much_x, much_dy = jax.random.uniform(kz, (2,), jnp.float32, 0.0, 1.0)
    loud = 2.0 ** jax.random.uniform(jax.random.fold_in(kz, 1), (), jnp.float32, -1.0, 2.0)
    layers = 2.0 ** jax.random.uniform(kl, (LAYERS, 1, 1), jnp.float32, -1.0, 1.0)
    x = together(ka, jax.random.normal(kx, shape, jnp.float32), much_x) * bump(kf, D, 4.0)
    dy = together(kb, jax.random.normal(kdy, shape, jnp.float32), much_dy)
    drawn = {"x": x.astype(jnp.bfloat16), "dy": (loud * dy * (SEQUENCES * TOKENS) ** -0.5).astype(jnp.bfloat16)}
    for key, name in zip(kw, NAMES, strict=True):
        w = jax.random.normal(key, SHAPES[name], jnp.float32) * SHAPES[name][1] ** -0.5
        drawn[name] = (w * {"w_gate": 1.0, "w_up": bump(kh, FF, 4.0), "w_down": layers}[name]).astype(jnp.bfloat16)
    for key, name in zip(km, NAMES, strict=True):
        drawn[f"m_{name}"] = 0.1 * jax.random.normal(key, SHAPES[name], jnp.float32)
    for key, name in zip(kv, NAMES, strict=True):
        drawn[f"v_{name}"] = jax.random.uniform(key, SHAPES[name], jnp.float32, 0.005, 0.015)
    return drawn


def matmul(a, w):
    return jnp.dot(a, w, preferred_element_type=jnp.float32).astype(jnp.bfloat16)


def normed(h):
    wide = h.astype(jnp.float32)
    scale = lax.rsqrt(jnp.mean(wide**2, -1, keepdims=True) + 1e-6)
    return (wide * scale).astype(jnp.bfloat16)


def layer(h, w):
    a = normed(h)
    gate = jnp.dot(a, w["w_gate"], preferred_element_type=jnp.float32)
    up = jnp.dot(a, w["w_up"], preferred_element_type=jnp.float32)
    return h + matmul((jax.nn.silu(gate) * up).astype(jnp.bfloat16), w["w_down"])


def adamw(w, m, v, g):
    m = 0.9 * m + 0.1 * g
    v = 0.95 * v + 0.05 * g * g
    step = m * lax.rsqrt(v + 1e-8) + 0.1 * w
    return (w - 0.02 * step).astype(jnp.bfloat16), m, v


def clipped(gradients, sum_of_squares, count):
    factor = jnp.minimum(1.0, 0.5 * lax.rsqrt(sum_of_squares / count + 1e-30))
    return [g * factor for g in gradients]


def stack(weights, h):
    return lax.scan(lambda h, w: (layer(h, w), None), h, weights)[0]


def reference(x, dy, w_gate, w_up, w_down, m_w_gate, m_w_up, m_w_down, v_w_gate, v_w_up, v_w_down):
    weights = dict(zip(NAMES, (w_gate, w_up, w_down), strict=True))

    def take(so_far, sequence):
        h, by_y = sequence
        _, back = jax.vjp(lambda w: stack(w, h), weights)
        return jax.tree.map(lambda total, term: total + term.astype(jnp.float32), so_far, back(by_y)[0]), None

    none_yet = {name: jnp.zeros(w.shape, jnp.float32) for name, w in weights.items()}
    by_weights, _ = lax.scan(take, none_yet, (x, dy))
    gradients = [by_weights[name].astype(jnp.bfloat16).astype(jnp.float32) for name in NAMES]
    gradients = clipped(gradients, sum(jnp.sum(g * g) for g in gradients), sum(g.size for g in gradients))
    new = [
        adamw(w.astype(jnp.float32), m, v, g)
        for w, m, v, g in zip((w_gate, w_up, w_down), (m_w_gate, m_w_up, m_w_down), (v_w_gate, v_w_up, v_w_down), gradients, strict=True)
    ]
    return tuple(one[which] for which in range(3) for one in new)
```

```python
import jax
import jax.numpy as jnp
from jax import lax
from jax.sharding import PartitionSpec as P

BF, F32 = jnp.bfloat16, jnp.float32
FACTOR_COUNT = 2 * 3 * 1536 * 4224


def dot(a, b, ca, cb):
    return lax.dot_general(a, b, (((ca,), (cb,)), ((), ())), preferred_element_type=F32)


def norm(h):
    wide = h.astype(F32)
    s = lax.rsqrt(jnp.mean(wide**2, -1, keepdims=True) + 1e-6)
    return (wide * s).astype(BF), s


def norm_back(da, h, s):
    wide, da = h.astype(F32), da.astype(F32)
    return s * (da - wide * (s * s) * jnp.mean(da * wide, -1, keepdims=True))


def gates(a, wg, wu):
    return dot(a, wg, 1, 0), dot(a, wu, 1, 0)


def product(gate, up):
    return (jax.nn.silu(gate) * up).astype(BF)


def product_back(gate, up, dp):
    sig = jax.nn.sigmoid(gate)
    dp = dp.astype(F32)
    dgate = dp * up * (sig * (1 + gate * (1 - sig)))
    dup = dp * (gate * sig)
    return dgate.astype(BF), dup.astype(BF)


def adamw(w, m, v, g):
    m = 0.9 * m + 0.1 * g
    v = 0.95 * v + 0.05 * g * g
    step = m * lax.rsqrt(v + 1e-8) + 0.1 * w
    return (w - 0.02 * step).astype(BF), m, v


def solution(mesh):
    def body(x, dy, wg, wu, wd, *mv):
        x, dy = x[0], dy[0]
        rs = lambda g: lax.psum_scatter(g, "dp", scatter_dimension=0, tiled=True)
        a0, s0 = norm(x)
        gate0, up0 = gates(a0, wg[0], wu[0])
        p0 = product(gate0, up0)
        h1 = x + dot(p0, wd[0], 1, 0).astype(BF)
        a1, s1 = norm(h1)
        gate1, up1 = gates(a1, wg[1], wu[1])
        p1 = product(gate1, up1)
        gd1 = rs(dot(p1, dy, 0, 0).astype(BF))
        dp1 = dot(dy, wd[1], 1, 1).astype(BF)
        dg1, du1 = product_back(gate1, up1, dp1)
        gg1 = rs(dot(a1, dg1, 0, 0).astype(BF))
        gu1 = rs(dot(a1, du1, 0, 0).astype(BF))
        da1 = (dot(dg1, wg[1], 1, 1) + dot(du1, wu[1], 1, 1)).astype(BF)
        dh1 = (dy.astype(F32) + norm_back(da1, h1, s1)).astype(BF)
        gd0 = rs(dot(p0, dh1, 0, 0).astype(BF))
        dp0 = dot(dh1, wd[0], 1, 1).astype(BF)
        dg0, du0 = product_back(gate0, up0, dp0)
        gg0 = rs(dot(a0, dg0, 0, 0).astype(BF))
        gu0 = rs(dot(a0, du0, 0, 0).astype(BF))
        grads = [jnp.stack([gg0, gg1]), jnp.stack([gu0, gu1]), jnp.stack([gd0, gd1])]
        grads = [g.astype(F32) for g in grads]
        total = lax.psum(sum(jnp.sum(g * g) for g in grads), "dp")
        factor = jnp.minimum(1.0, 0.5 * lax.rsqrt(total / FACTOR_COUNT + 1e-30))
        me = lax.axis_index("dp")
        ws = []
        for w in (wg, wu, wd):
            rows = w.shape[1] // 16
            ws.append(lax.dynamic_slice_in_dim(w, me * rows, rows, 1))
        new = [adamw(w.astype(F32), m, v, g * factor) for w, m, v, g in zip(ws, mv[:3], mv[3:], grads)]
        full = [lax.all_gather(n[0], "dp", axis=1, tiled=True) for n in new]
        return (*full, *(n[1] for n in new), *(n[2] for n in new))

    seq, whole, block = P(("rep", "dp"), None, None), P(None, None, None), P(None, "dp", None)
    out_whole, out_block = P("rep", None, None), P("rep", "dp", None)
    return jax.shard_map(
        body, mesh=mesh,
        in_specs=(seq, seq, whole, whole, whole, *(block,) * 6),
        out_specs=(out_whole,) * 3 + (out_block,) * 6,
        check_vma=False,
    )
```
